32 devices in a mesh: ctx: 4 (over y, core), exp: 8 (over z, x).
Axes of the slice: x: 2, y: 2, z: 4, core: 2. Of those that a mesh axis runs over, the one named last changes fastest.
Arguments:
- queries: bfloat16 [512, 8192], P('ctx', 'exp'), may hold values from -4 to 4
- keys: bfloat16 [512, 512], P('ctx'), may hold values from -4 to 4
- values: bfloat16 [512, 512], P('ctx'), may hold values from -4 to 4
- stretch_order: int32 [8], replicated, may hold values from 0 to 7, each once
- attention_proj: bfloat16 [8192, 4096], P('exp'), may hold values from -0.0625 to 0.0625
- out_grad: bfloat16 [512, 4096], P(('ctx', 'exp')), may hold values from -6 to 6
- expert_outputs: bfloat16 [512, 8, 4096], P(('ctx', 'exp')), may hold values from -0.28125 to 0.28125
- route_logits: float32 [512, 8], P(('ctx', 'exp')), may hold values from -8 to 250
- routes: int32 [512, 8], P(('ctx', 'exp')), may hold values from 0 to 127, as said below
- router_weight: bfloat16 [4096, 128], replicated, may hold values from -3 to 3
Outputs:
- query_grad: bfloat16 [512, 8192], P('ctx', 'exp')
- logit_grad: float32 [512, 8], P(('ctx', 'exp'))
- slot_grads: bfloat16 [4, 8, 8, 32, 4096], P('ctx', 'exp')
The draws below stay inside these ranges and needn't reach their ends.
Inputs may be any that keep to these rules, and one draw needn't show every extreme that they name: `routes`: each row names 8 different experts. Owner o holds experts o * 16 to (o + 1) * 16 - 1. In the rows of one device (aligned blocks of 16 rows), the block's entries name experts of one owner at most 32 times, and some owner exactly 32 times, in every block.
All inputs are finite; a program needn't handle non-finite values.
Results may differ from the reference program's by a relative error of at most 0.013.
Values may be sent and summed in bfloat16 or wider, within the bound.
No kernel may reach another device: no remote copies, remote signals or barrier semaphores. Data moves between devices by JAX's collectives and lax.ppermute only.
A program may use at most 64 MiB of HBM per device.

```python
import math
import jax
import jax.numpy as jnp
from jax import lax

D = 4096
QUERY_HEADS = 64
KEY_VALUE_HEADS = 4
HEAD_WIDTH = 128
EXPERTS = 128
TOP = 8
SEQUENCE_TOKENS = 512
HALF = 64
STRETCHES = 8
MOE_DEV = 16
EXP_DEV = 16
SLOTS = 32
N_CTX = 4
N_EXP = 8


def paired_rows(key):
    base = jax.random.fold_in(key, 5)
    first, second_operand = jax.random.split(base, 2)
    upper_limit = float(4 + (128 // HEAD_WIDTH - 1) * 2 // 3)
    queries = jnp.clip(jax.random.normal(first, (SEQUENCE_TOKENS, QUERY_HEADS, HEAD_WIDTH), jnp.float32), -upper_limit, upper_limit)
    keys = jnp.clip(jax.random.normal(second_operand, (SEQUENCE_TOKENS, KEY_VALUE_HEADS, HEAD_WIDTH), jnp.float32), -upper_limit, upper_limit)
    return (queries.reshape(SEQUENCE_TOKENS, QUERY_HEADS * HEAD_WIDTH), keys.reshape(SEQUENCE_TOKENS, KEY_VALUE_HEADS * HEAD_WIDTH))


def draw_queries(key, part):
    return paired_rows(key)[0].astype(jnp.bfloat16)


def draw_keys(key, part):
    return paired_rows(key)[1].astype(jnp.bfloat16)


def draw_route_logits(key, part):
    first = jax.random.fold_in(jax.random.fold_in(key, 9), 0)
    logits = jnp.clip(1.5 * jax.random.normal(first, (SEQUENCE_TOKENS, TOP), jnp.float32), -8.0, 8.0)
    return logits


def draw_routes(key, part):
    owners = EXPERTS // EXP_DEV
    pair_rows = MOE_DEV * TOP
    blocks = SEQUENCE_TOKENS // MOE_DEV

    def one_block(block_key):
        first, second_operand, third, fourth_operand = jax.random.split(block_key, 4)
        forced = jax.random.randint(first, (), 0, owners)
        shuffled = jax.random.permutation(second_operand, owners * SLOTS)
        holder = shuffled // SLOTS
        ranking = jnp.where(holder == forced, 0, 1) * (owners * SLOTS) + jnp.arange(owners * SLOTS, dtype=jnp.int32)
        ordered = holder[jnp.argsort(ranking, stable=True)]
        chosen = jax.random.permutation(third, ordered[:pair_rows]).reshape(MOE_DEV, TOP)
        same = (chosen[:, :, None] == chosen[:, None, :]).astype(jnp.int32)
        earlier = jnp.sum(jnp.tril(same, -1), axis=2)
        offsets = jax.random.randint(fourth_operand, (MOE_DEV, owners), 0, EXP_DEV)
        starting = jnp.take_along_axis(offsets, chosen, axis=1)
        inside = (starting + earlier) % EXP_DEV
        return chosen * EXP_DEV + inside
    block_keys = jax.random.split(jax.random.fold_in(key, 13), blocks)
    return jax.vmap(one_block)(block_keys).reshape(SEQUENCE_TOKENS, TOP).astype(jnp.int32)


def level_of(key, dims, cuts, least, top_value):
    gain = 1.0
    for dim, shards_of in cuts:
        heights = jax.random.uniform(jax.random.fold_in(jax.random.fold_in(key, 6), dim), (shards_of,), jnp.float32, least / len(cuts), top_value / len(cuts))
        gain = gain * jnp.repeat(jnp.exp(heights), dims[dim] // shards_of).reshape((-1,) + (1,) * (len(dims) - 1 - dim))
    return gain


def centred(key, shape, spread, bound, shards=(), held_as=jnp.bfloat16):
    drawn = jax.random.normal(key, shape, jnp.float32) * spread
    if len(shards) > 0:
        drawn = level_of(key, shape, shards, -0.22, 0.18) * drawn
    return jnp.clip(drawn, min=-bound, max=bound).astype(held_as)


def setup_inputs(seed: int = 0) -> dict:
    key_of = jax.random.split(jax.random.key(seed), 11)
    return {
        "queries": draw_queries(jax.random.fold_in(key_of[10], 71), 0),
        "keys": draw_keys(jax.random.fold_in(key_of[10], 71), 0),
        "values": centred(key_of[2], (SEQUENCE_TOKENS, KEY_VALUE_HEADS * HEAD_WIDTH), 1.0, 4.0, ((0, 4),)),
        "stretch_order": jax.random.permutation(key_of[3], STRETCHES).astype(jnp.int32),
        "attention_proj": centred(key_of[4], (QUERY_HEADS * HEAD_WIDTH, D), (QUERY_HEADS * HEAD_WIDTH) ** -0.5, 0.0625, ((0, 8),)),
        "out_grad": centred(key_of[5], (SEQUENCE_TOKENS, D), 1.0, 6.0, ((0, 32),)),
        "expert_outputs": centred(key_of[6], (SEQUENCE_TOKENS, TOP, D), (3.0 / D ** 0.5), 0.28125, ((0, 32),)),
        "route_logits": draw_route_logits(jax.random.fold_in(key_of[10], 71), 0),
        "routes": draw_routes(jax.random.fold_in(key_of[10], 71), 0),
        "router_weight": centred(key_of[9], (D, EXPERTS), 0.5, 3.0),
    }


YARN_BASE = 0.1 * math.log(4.0) + 1.0

def reference(queries, keys, values, stretch_order, attention_proj, out_grad, expert_outputs, route_logits, routes, router_weight):
    scale = YARN_BASE ** 2 / math.sqrt(HEAD_WIDTH)
    gates = jax.nn.softmax(route_logits, axis=-1)
    grad_wide = out_grad.astype(jnp.float32)
    weighted = (gates[:, :, None] * grad_wide[:, None, :]).astype(jnp.bfloat16)
    gate_grad = jnp.einsum('md,mkd->mk', grad_wide, expert_outputs.astype(jnp.float32))
    logit_grad = gates * (gate_grad - lax.optimization_barrier(jnp.sum(gates * gate_grad, axis=1, keepdims=True)))
    experts = jnp.arange(EXPERTS, dtype=jnp.int32)
    picks = (routes[:, :, None] == experts[None, None, :]).astype(jnp.float32)
    route_grad = lax.optimization_barrier(jnp.sum(picks * logit_grad[:, :, None], axis=1)).astype(jnp.bfloat16)
    through = jnp.dot(route_grad, router_weight.T, preferred_element_type=jnp.float32)
    residual_grad = (grad_wide + through).astype(jnp.bfloat16)
    head_grad = jnp.dot(residual_grad, attention_proj.T, preferred_element_type=jnp.float32).astype(jnp.bfloat16)
    per_owner = EXPERTS // N_EXP
    pair_rows = MOE_DEV * TOP
    block_routes = routes.reshape(N_CTX, N_EXP, pair_rows)
    block_values = weighted.reshape(N_CTX, N_EXP, pair_rows, D)

    def pack_ctx(item):
        route_set, value_set = item
        owners = route_set // per_owner
        marks = (owners[:, :, None] == jnp.arange(N_EXP, dtype=jnp.int32)[None, None, :]).astype(jnp.int32)
        earlier = lax.optimization_barrier(jnp.sum((jnp.cumsum(marks, axis=1) - marks) * marks, axis=2))
        target = owners * SLOTS + earlier
        placing = (jnp.arange(N_EXP * SLOTS, dtype=jnp.int32)[None, :, None] == target[:, None, :]).astype(jnp.float32)
        packed = jnp.einsum('sjr,srd->sjd', placing, value_set.astype(jnp.float32)).astype(jnp.bfloat16)
        return packed.reshape(N_EXP, N_EXP, SLOTS, D).transpose(1, 0, 2, 3)
    slot_grads = lax.map(pack_ctx, (block_routes, block_values))
    index = jnp.arange(SEQUENCE_TOKENS, dtype=jnp.int32)
    pos = stretch_order[index // HALF] * HALF + index % HALF
    allowed = pos[None, :] <= pos[:, None]
    query_heads = queries.reshape(SEQUENCE_TOKENS, QUERY_HEADS, HEAD_WIDTH)
    key_head_rows = keys.reshape(SEQUENCE_TOKENS, KEY_VALUE_HEADS, HEAD_WIDTH)
    value_head_rows = values.reshape(SEQUENCE_TOKENS, KEY_VALUE_HEADS, HEAD_WIDTH)
    grad_heads = head_grad.reshape(SEQUENCE_TOKENS, QUERY_HEADS, HEAD_WIDTH)
    head_group = QUERY_HEADS // KEY_VALUE_HEADS

    def one_head(head):
        query_h = lax.dynamic_index_in_dim(query_heads, head, 1, keepdims=False)
        grad_h = lax.dynamic_index_in_dim(grad_heads, head, 1, keepdims=False)
        key_h = lax.dynamic_index_in_dim(key_head_rows, head // head_group, 1, keepdims=False)
        value_h = lax.dynamic_index_in_dim(value_head_rows, head // head_group, 1, keepdims=False)
        scores = scale * jnp.dot(query_h, key_h.T, preferred_element_type=jnp.float32)
        scores = jnp.where(allowed, scores, -jnp.inf)
        totals = jax.nn.logsumexp(scores, axis=1)
        probs = jnp.exp(scores - totals[:, None])
        attn_out = jnp.dot(probs.astype(jnp.bfloat16), value_h, preferred_element_type=jnp.float32)
        delta = lax.optimization_barrier(jnp.sum(grad_h.astype(jnp.float32) * attn_out, axis=1))
        prob_grad = jnp.dot(grad_h, value_h.T, preferred_element_type=jnp.float32)
        score_grad = (probs * (prob_grad - delta[:, None])).astype(jnp.bfloat16)
        return (scale * jnp.dot(score_grad, key_h, preferred_element_type=jnp.float32)).astype(jnp.bfloat16)
    per_head = lax.map(one_head, jnp.arange(QUERY_HEADS, dtype=jnp.int32))
    query_grad = per_head.transpose(1, 0, 2).reshape(SEQUENCE_TOKENS, QUERY_HEADS * HEAD_WIDTH)
    return (query_grad, logit_grad, slot_grads)
```

```python
import math

import jax
import jax.numpy as jnp
from jax import lax
from jax.experimental import pallas as pl
from jax.experimental.pallas import tpu as pltpu
from jax.sharding import PartitionSpec as P

QUERY_HEADS = 64
KEY_VALUE_HEADS = 4
HEAD_WIDTH = 128
EXPERTS = 128
TOP = 8
LANES = 128

YARN_BASE = 0.1 * math.log(4.0) + 1.0
SCALE = YARN_BASE**2 / math.sqrt(HEAD_WIDTH)
NEG_FILL = -1e30
F32 = jnp.float32
BF16 = jnp.bfloat16
NT = (((1,), (1,)), ((), ()))
VMEM = pl.BlockSpec(memory_space=pltpu.VMEM)
SMEM = pl.BlockSpec(memory_space=pltpu.SMEM)


def dot(a, b, dims=None, **kw):
    if dims is None:
        dims = (((1,), (0,)), ((), ()))
    return lax.dot_general(a, b, dims, preferred_element_type=F32, **kw)


def iota(shape, axis):
    return lax.broadcasted_iota(jnp.int32, shape, axis)


def gate_kernel(og_ref, eo_ref, logits_ref, routes_ref, packed_ref, logit_grad_ref):
    tokens, width = og_ref.shape
    pairs = tokens * TOP
    og = og_ref[...]
    crossed = dot(og, eo_ref[...], NT)
    own = iota((tokens, pairs), 1) // TOP == iota((tokens, pairs), 0)
    fold = (iota((pairs, TOP), 0) % TOP == iota((pairs, TOP), 1)).astype(F32)
    gate_grad = dot(jnp.where(own, crossed, 0.0), fold, precision=lax.Precision.HIGHEST)
    logits = logits_ref[...]
    weights = jnp.exp(logits - jnp.max(logits, axis=1, keepdims=True))
    gates = weights / jnp.sum(weights, axis=1, keepdims=True)
    logit_grad = gates * (gate_grad - jnp.sum(gates * gate_grad, axis=1, keepdims=True))
    logit_grad_ref[...] = logit_grad
    routes = routes_ref[...]
    expert = iota((tokens, EXPERTS), 1)
    route_grad = jnp.zeros((tokens, EXPERTS), F32)
    for k in range(TOP):
        route_grad = route_grad + jnp.where(
            routes[:, k : k + 1] == expert, logit_grad[:, k : k + 1], 0.0
        )
    high = gates.astype(BF16)
    rest = gates - high.astype(F32)
    middle = rest.astype(BF16)
    low = (rest - middle.astype(F32)).astype(BF16)
    small = jnp.zeros((tokens, LANES), F32)
    for i, part in enumerate((routes.astype(F32).astype(BF16), high, middle, low)):
        spot = (iota((TOP, LANES), 0) + TOP * i == iota((TOP, LANES), 1)).astype(BF16)
        small = small + dot(part, spot)
    packed_ref[:, :width] = og
    packed_ref[:, width : width + LANES] = small.astype(BF16)
    packed_ref[:, width + LANES :] = route_grad.astype(BF16)


def forward_kernel(order_ref, flip_ref, q_ref, *refs):
    pieces, (probs_ref, out_ref) = refs[:-2], refs[-2:]
    tokens = q_ref.shape[0]
    heads = q_ref.shape[1] // HEAD_WIDTH
    half = tokens // 2
    mine = flip_ref[0]
    k = jnp.concatenate([r[:, :HEAD_WIDTH] for r in pieces], axis=0)
    v = jnp.concatenate([r[:, HEAD_WIDTH:] for r in pieces], axis=0)
    blocks = k.shape[0] // tokens
    row = iota((tokens, LANES), 0)
    row = jnp.where(
        row < half,
        order_ref[2 * mine] * half + row,
        order_ref[2 * mine + 1] * half + row - half,
    )
    biases = []
    for b in range(blocks):
        source = b ^ flip_ref[1]
        lane = iota((tokens, tokens), 1)
        lane = jnp.where(
            lane < half,
            order_ref[2 * source] * half + lane,
            order_ref[2 * source + 1] * half + lane - half,
        )
        biases.append(jnp.where(lane <= row[:, :1], 0.0, NEG_FILL))
    bias = jnp.concatenate(biases, axis=1)
    for h in range(heads):
        raw = dot(q_ref[:, h * HEAD_WIDTH : (h + 1) * HEAD_WIDTH], k, NT)
        raw = raw * SCALE + bias
        weights = jnp.exp(raw - jnp.max(raw, axis=1, keepdims=True))
        probs = weights / jnp.sum(weights, axis=1, keepdims=True)
        probs = probs.astype(BF16)
        probs_ref[h] = probs
        out_ref[h] = dot(probs, v)


def tail_kernel(n_blocks, n_pieces, slots, flip_ref, *refs):
    blocks = refs[:n_blocks]
    pieces = refs[n_blocks : n_blocks + n_pieces]
    w_ref, rw_ref, probs_ref, out_ref, query_grad_ref, slot_ref = refs[n_blocks + n_pieces :]
    width = w_ref.shape[1]
    heads = probs_ref.shape[0]
    tokens = probs_ref.shape[1]
    sources = slot_ref.shape[0] // slots
    each = tokens // sources
    me = flip_ref[0]
    flip = flip_ref[1]
    og = jnp.concatenate([r[:, :width] for r in blocks], axis=0)
    small = jnp.concatenate([r[:, width : width + LANES] for r in blocks], axis=0)
    route_grad = jnp.concatenate([r[:, width + LANES :] for r in blocks], axis=0)
    through = dot(route_grad, rw_ref[...], NT)
    residual = (og.astype(F32) + through).astype(BF16)
    turned = dot(w_ref[...], residual, NT).astype(BF16)
    r, c = iota((tokens, tokens), 0), iota((tokens, tokens), 1)
    unmix = ((r // each) ^ flip == c // each) & (r % each == c % each)
    head_grad = dot(unmix.astype(BF16), turned, NT).astype(BF16)
    k = jnp.concatenate([r[:, :HEAD_WIDTH] for r in pieces], axis=0)
    v = jnp.concatenate([r[:, HEAD_WIDTH:] for r in pieces], axis=0)
    for h in range(heads):
        cols = slice(h * HEAD_WIDTH, (h + 1) * HEAD_WIDTH)
        grad = head_grad[:, cols]
        delta = jnp.sum(grad.astype(F32) * out_ref[h], axis=1, keepdims=True)
        prob_grad = dot(grad, v, NT)
        score_grad = (probs_ref[h].astype(F32) * (prob_grad - delta)).astype(BF16)
        query_grad_ref[:, cols] = (SCALE * dot(score_grad, k)).astype(BF16)
    across = small.astype(F32).T
    routes = across[:TOP].astype(jnp.int32)
    gates = across[TOP : 2 * TOP] + across[2 * TOP : 3 * TOP] + across[3 * TOP : 4 * TOP]
    mark = routes // (EXPERTS // sources) == me
    marks = mark.astype(F32).astype(BF16)
    counts = jnp.sum(mark.astype(F32), axis=0, keepdims=True)
    before = ((r // each == c // each) & (r < c)).astype(F32).astype(BF16)
    counts = jnp.broadcast_to(counts, (TOP, tokens)).astype(BF16)
    lower = (iota((TOP, TOP), 1) < iota((TOP, TOP), 0)).astype(F32).astype(BF16)
    earlier = (dot(counts, before) + dot(lower, marks)).astype(jnp.int32)
    source = (iota((TOP, tokens), 1) // each) ^ flip
    target = jnp.where(mark, source * slots + earlier, -1)
    spot = iota((slot_ref.shape[0], tokens), 0)
    chosen = jnp.zeros(spot.shape, F32)
    weight = jnp.zeros(spot.shape, F32)
    for j in range(TOP):
        hit = spot == target[j : j + 1]
        chosen = jnp.where(hit, 1.0, chosen)
        weight = jnp.where(hit, gates[j : j + 1], weight)
    weight = jnp.sum(weight, axis=1, keepdims=True)
    slot_ref[...] = (dot(chosen.astype(BF16), og) * weight).astype(BF16)


def swap(x, axis, offset):
    return lax.ppermute(x, axis, [(i, i ^ offset) for i in range(lax.axis_size(axis))])


def exchange(x, axis):
    n = lax.axis_size(axis)
    if n & (n - 1) or n > 8:
        return [lax.all_gather(x, axis, axis=0, tiled=True)], jnp.int32(0)
    got = {0: x}
    direct = [k for k in range(1, n) if k & (k - 1) == 0 or k == n - 1]
    for k in sorted(direct, key=lambda k: (-(k.bit_length()), -k)):
        got[k] = swap(x, axis, k)
    for k in range(n - 1, 0, -1):
        if k not in got:
            low = k & -k
            got[k] = swap(got[k - low], axis, low)
    return [got[k] for k in range(n)], lax.axis_index(axis).astype(jnp.int32)


def on_device(
    queries,
    keys,
    values,
    stretch_order,
    attention_proj,
    out_grad,
    expert_outputs,
    route_logits,
    routes,
    router_weight,
):
    tokens = queries.shape[0]
    moe_tokens, width = out_grad.shape
    heads = queries.shape[1] // HEAD_WIDTH
    sources = lax.axis_size("exp")
    slots = max(2, 2 * moe_tokens * TOP // sources)
    params = pltpu.CompilerParams(vmem_limit_bytes=40 * 2**20)
    sds = jax.ShapeDtypeStruct
    packed, logit_grad = pl.pallas_call(
        gate_kernel,
        name="gates",
        out_shape=(sds((moe_tokens, width + 2 * LANES), BF16), sds((moe_tokens, TOP), F32)),
        in_specs=[VMEM] * 4,
        out_specs=(VMEM, VMEM),
        compiler_params=params,
    )(out_grad, expert_outputs.reshape(moe_tokens * TOP, width), route_logits, routes)
    blocks, flip = exchange(packed, "exp")

    head_group = QUERY_HEADS // KEY_VALUE_HEADS
    kv_head = lax.axis_index("exp") * heads // head_group
    own = jnp.concatenate(
        [
            lax.dynamic_slice_in_dim(x, kv_head * HEAD_WIDTH, HEAD_WIDTH, 1)
            for x in (keys, values)
        ],
        axis=1,
    )
    pieces, key_flip = exchange(own, "ctx")
    mine = lax.axis_index("ctx").astype(jnp.int32)
    total = sum(p.shape[0] for p in pieces)
    probs, attn_out = pl.pallas_call(
        forward_kernel,
        name="forward",
        out_shape=(sds((heads, tokens, total), BF16), sds((heads, tokens, HEAD_WIDTH), F32)),
        in_specs=[SMEM, SMEM, VMEM] + [VMEM] * len(pieces),
        out_specs=(VMEM, VMEM),
        compiler_params=params,
    )(stretch_order, jnp.stack([mine, key_flip]), queries, *pieces)

    me = lax.axis_index("exp").astype(jnp.int32)
    query_grad, slot_rows = pl.pallas_call(
        lambda *refs: tail_kernel(len(blocks), len(pieces), slots, *refs),
        name="tail",
        out_shape=(sds(queries.shape, BF16), sds((sources * slots, width), BF16)),
        in_specs=[SMEM] + [VMEM] * (len(blocks) + len(pieces) + 4),
        out_specs=(VMEM, VMEM),
        compiler_params=params,
    )(jnp.stack([me, flip]), *blocks, *pieces, attention_proj, router_weight, probs, attn_out)
    return (query_grad, logit_grad, slot_rows.reshape(1, 1, sources, slots, width))


def solution(mesh):
    in_specs = (
        P("ctx", "exp"),
        P("ctx", None),
        P("ctx", None),
        P(),
        P("exp", None),
        P(("ctx", "exp"), None),
        P(("ctx", "exp"), None, None),
        P(("ctx", "exp"), None),
        P(("ctx", "exp"), None),
        P(),
    )
    out_specs = (P("ctx", "exp"), P(("ctx", "exp"), None), P("ctx", "exp", None, None, None))
    return jax.shard_map(
        on_device, mesh=mesh, in_specs=in_specs, out_specs=out_specs, check_vma=False
    )
```
